32 devices in a mesh: gx: 4 (over y, x), gy: 4 (over z), gz: 2 (over core).
Axes of the slice: x: 2, y: 2, z: 4, core: 2. Of those that a mesh axis runs over, the one named last changes fastest.
Arguments:
- token_grad: bfloat16 [32768, 320], P(('gx', 'gy', 'gz')), may hold values from -6 to 6
- token_owner: int32 [32768, 1], P(('gx', 'gy', 'gz')), may hold values from 0 to 31; in each aligned block of 1024 rows (0 to 1023, 1024 to 2047, ...) at most 64 rows name the same one
- token_row: int32 [32768], P(('gx', 'gy', 'gz')), may hold values from 0 to 4095
- table: float32 [131072, 320], P(('gx', 'gy', 'gz')), may hold values from -6 to 6
- accum: float32 [131072], P(('gx', 'gy', 'gz')), may hold values from 0.1 to 10
Outputs:
- new_table: float32 [131072, 320], P(('gx', 'gy', 'gz'))
- new_accum: float32 [131072], P(('gx', 'gy', 'gz'))
- fresh_rows: bfloat16 [32768, 320], P(('gx', 'gy', 'gz'))
The draws below stay inside these ranges and needn't reach their ends.
Inputs may be any that keep to these rules, and one draw needn't show every extreme that they name: `token_owner`: among the 1024 tokens of one device no owner is named by more than 64 tokens.
All inputs are finite; a program needn't handle non-finite values.
Results may differ from the reference program's by a relative error of at most 0.001.
Values may be sent and summed in bfloat16 or wider, within the bound.
A program may use at most 64 MiB of HBM per device.

```python
import math
import jax
import jax.numpy as jnp
import numpy as np
from jax import lax

W = 320
ROWS_DEV = 4096
TOK_DEV = 1024
OWNERS = 32
CAP = 64
TOKENS = 32768
ROWS = 131072


def plant(drawn, stream_key, low, largest):
    spot = [jax.random.randint(jax.random.fold_in(stream_key, axis), (), 0, length) for axis, length in enumerate(drawn.shape)]
    main_axis = drawn.shape.index(max(drawn.shape))
    next_to = spot[:main_axis] + [(spot[main_axis] + 1) % drawn.shape[main_axis]] + spot[main_axis + 1:]
    return drawn.at[tuple(spot)].set(low).at[tuple(next_to)].set(largest)


def levels(stream_key, dims, pieces, low, largest):
    gain, own = 1.0, jax.random.fold_in(stream_key, 6)
    for axis_at, blocks in pieces:
        draws = jnp.exp(jax.random.uniform(jax.random.fold_in(own, axis_at), (blocks,), jnp.float32, low / len(pieces), largest / len(pieces)))
        gain = gain * jnp.repeat(draws, dims[axis_at] // blocks).reshape([-1 if axis == axis_at else 1 for axis in range(len(dims))])
    return gain


def rank_table(number_of, lean):
    portions = [(1 << 20) // math.isqrt(rank ** lean) + 1 for rank in range(1, number_of + 1)]
    spread = 1 + sum(portions) // (1 << 30)
    return np.cumsum(np.array([max(1, weight // spread) for weight in portions]))


def ranked_ids(key, shape, number_of, slope):
    listing = rank_table(number_of, slope)
    lot = jax.random.randint(jax.random.fold_in(key, 1), shape, 0, int(listing[number_of - 1]))
    grade = jnp.searchsorted(jnp.asarray(listing, jnp.int32), lot, side="right")
    return jax.random.permutation(jax.random.fold_in(key, 2), number_of)[grade].astype(jnp.int32)


def routed_block(stream_key, own, number, rows, amount, top, reach, skew):
    ranking = jax.random.permutation(stream_key, amount)
    crowded, usual = load_shares(amount, rows * top, reach, skew, True), load_shares(amount, rows * top, reach, skew, False)
    places = jnp.arange(amount)

    def named(lengths, turn):
        used = int((lengths > 0).sum())
        fixed = max(1, used // 4)
        moved = fixed + (places - fixed + turn * (used - fixed)) % max(1, amount - fixed)
        return jnp.zeros((amount,), jnp.int32).at[ranking[jnp.where(places < fixed, places, moved)]].set(jnp.asarray(lengths, jnp.int32))

    lengths = jnp.where(number % 4 == 0, named(crowded, number // 4), named(usual, number - number // 4 - 1))
    mixed = jax.random.permutation(jax.random.fold_in(own, 3), amount)
    giver, receiver = mixed[0:amount // 2 * 2:2], mixed[1:amount // 2 * 2:2]
    margin = jnp.minimum(lengths[giver] - 1, reach - lengths[receiver]) // 2
    margin = jnp.where((giver == ranking[0]) | (receiver == ranking[0]) | (lengths[receiver] == 0), 0, jnp.maximum(margin, 0))
    moved = jax.random.randint(jax.random.fold_in(own, 4), (amount // 2,), 0, 1 << 20) % (margin + 1)
    lengths = lengths.at[giver].add(-moved).at[receiver].add(moved)
    members = jnp.searchsorted(jnp.cumsum(lengths), jnp.arange(rows * top), side="right").astype(jnp.int32)
    listing = members.reshape(top, rows).T
    listing = listing[jax.random.permutation(jax.random.fold_in(own, 1), rows)]
    turn = jax.random.randint(jax.random.fold_in(own, 2), (rows, 1), 0, top)
    return jnp.take_along_axis(listing, (jnp.arange(top)[None, :] + turn) % top, axis=1)


def load_shares(count, total, most, lean, full):
    weights = [(1 << 20) // math.isqrt(grade ** lean) + 1 for grade in range(1, count + 1)]
    largest = most if full else min(most, max(-(-total // count), total * weights[0] // sum(weights)))
    least = 1 if total - largest >= count - 1 else 0
    given, surplus = [largest] + [least] * (count - 1), total - largest - least * (count - 1)
    while surplus > 0:
        free = [i for i in range(1, count) if given[i] < largest] or [i for i in range(1, count) if given[i] < most]
        mass, budget = sum([weights[i] for i in free]), surplus
        for i in free:
            more = min(most - given[i], max(1, budget * weights[i] // mass), surplus)
            given[i] = given[i] + more
            surplus = surplus - more
    return np.array(given)


def normal_values(key, dims, width, most, cuts=(), kind=jnp.bfloat16):
    drawn = jax.random.normal(key, dims, jnp.float32) * width
    if len(cuts) > 0:
        drawn = levels(key, dims, cuts, -0.22, 0.18) * drawn
    return jnp.clip(drawn, min=-most, max=most).astype(kind)


def setup_inputs(seed: int = 0) -> dict:
    key_of = jax.random.split(jax.random.key(seed), 6)
    token_grad = normal_values(key_of[0], (TOKENS, W), 1.0, 6.0, ((0, 32),))
    token_owner_keys = jax.random.split(jax.random.fold_in(key_of[1], 1), TOKENS // TOK_DEV)
    token_owner_turns = jax.random.permutation(jax.random.fold_in(key_of[1], 3), TOKENS // TOK_DEV)
    token_owner = jax.vmap(lambda own, number: routed_block(jax.random.fold_in(key_of[1], 2), own, number, TOK_DEV, OWNERS, 1, CAP, 2))(token_owner_keys, token_owner_turns).reshape((TOKENS, 1))
    token_row = plant(ranked_ids(key_of[2], (TOKENS,), ROWS_DEV, 2), jax.random.fold_in(key_of[2], 3), 0, ROWS_DEV - 1).astype(jnp.int32)
    table = normal_values(key_of[3], (ROWS, W), 1.0, 6.0, ((0, 32),), jnp.float32)
    accum = jnp.clip(jnp.exp(math.log(10.0) - 4.6051702 * jax.random.uniform(key_of[4], (ROWS,), jnp.float32) ** levels(key_of[4], (ROWS,), ((0, 32),), -0.2, 0.2)), 0.1, 10.0)
    return {"token_grad": token_grad, "token_owner": token_owner, "token_row": token_row, "table": table, "accum": accum}


def reference(token_grad, token_owner, token_row, table, accum):
    owners = token_owner[:, 0]
    gradients = token_grad.astype(jnp.float32)
    tables = table.reshape(OWNERS, ROWS_DEV, W)
    accums = accum.reshape(OWNERS, ROWS_DEV)

    def update(packed):
        owner_index, table_block, accum_block = packed
        is_mine = owners == owner_index
        segment_ids = jnp.where(is_mine, token_row, ROWS_DEV).astype(jnp.int32)
        summed = jax.ops.segment_sum(jnp.where(is_mine[:, None], gradients, jnp.float32(0.0)), segment_ids, num_segments=ROWS_DEV + 1)[:ROWS_DEV]
        grown = accum_block + lax.optimization_barrier(jnp.mean(summed * summed, axis=1))
        moved = table_block - 0.5 * summed / (jnp.sqrt(grown) + 1e-08)[:, None]
        return (moved, grown)
    new_tables, new_accums = lax.map(update, (jnp.arange(OWNERS, dtype=jnp.int32), tables, accums))
    new_table = new_tables.reshape(OWNERS * ROWS_DEV, W)
    new_accum = new_accums.reshape(OWNERS * ROWS_DEV)
    row_id = (owners * ROWS_DEV + token_row).astype(jnp.int32)
    fresh_rows = jnp.take(new_table, row_id, axis=0).astype(jnp.bfloat16)
    return (new_table, new_accum, fresh_rows)
```

```python
import functools

import jax
import jax.numpy as jnp
from jax import lax
from jax.experimental import pallas as pl
from jax.experimental.pallas import tpu as pltpu
from jax.sharding import PartitionSpec as P

AXES = ("gx", "gy", "gz")
BF, F32 = jnp.bfloat16, jnp.float32
MESH = pl.DeviceIdType.MESH


def iota(shape, axis):
    return lax.broadcasted_iota(jnp.int32, shape, axis).astype(F32)


def floor_div(value, by):
    return jnp.floor((value + 0.5) * (1.0 / by))


def onehot(column, line):
    return jnp.where(column == line, 1.0, 0.0).astype(BF)


def nt(left, right):
    return lax.dot_general(left, right, (((1,), (1,)), ((), ())), preferred_element_type=F32)


def kernel(sizes, half, grad_ref, owner_ref, row_ref, table_ref, accum_ref,
           new_table_ref, new_accum_ref, fresh_ref,
           ext_a, ext_b, send, recv, total, table, new_table, new_a, new_b,
           lhs, ans_a, ans_b, answer, returned, fresh,
           send_sem, recv_sem, back_sem, ret_sem, table_sem, out_sem):
    xs, ys, zs = sizes
    n = xs * ys * zs
    width, tokens = grad_ref.shape
    rows = table.shape[1]
    main = width // 128 * 128
    tail = width - main
    group = max(1, 256 // half)
    groups = n // group
    gs = group * half
    step_self = (ys - 1) * xs * zs
    me = tuple(lax.axis_index(axis) for axis in AXES)

    def delta(step):
        b = ys - 1 - step // (xs * zs)
        return lax.rem(step // zs, xs), b, lax.rem(step, zs)

    def ahead(step):
        return tuple(lax.rem(m + d, s) for m, d, s in zip(me, delta(step), sizes))

    def behind(step):
        return tuple(lax.rem(m + s - d, s) for m, d, s in zip(me, delta(step), sizes))

    barrier = pltpu.get_barrier_semaphore()

    def greet(step, carry):
        @pl.when(step != step_self)
        def _():
            pl.semaphore_signal(barrier, inc=1, device_id=ahead(step), device_id_type=MESH)
        return carry

    lax.fori_loop(0, n, greet, 0)
    load = pltpu.make_async_copy(table_ref, table, table_sem)
    load.start()

    owner = owner_ref[...].astype(F32)
    step = iota((n, tokens), 0)
    b_part = floor_div(step, xs * zs)
    rest = step - b_part * (xs * zs)
    a_part = floor_div(rest, zs)
    c_part = rest - a_part * zs
    b_part = ys - 1 - b_part

    def turn(part, m, size):
        moved = part + m.astype(F32)
        return jnp.where(moved >= size, moved - size, moved)

    named = (turn(a_part, me[0], xs) * ys + turn(b_part, me[1], ys)) * zs + turn(c_part, me[2], zs)
    match = jnp.where(named == owner, 1.0, 0.0)
    earlier = jnp.where(iota((tokens, tokens), 0) < iota((tokens, tokens), 1), 1.0, 0.0).astype(BF)
    before = jnp.dot(match.astype(BF), earlier, preferred_element_type=F32)
    rank = jnp.sum(match * before, axis=0, keepdims=True)
    base = jnp.sum(match * step, axis=0, keepdims=True) * half
    in_a = rank < half
    pos_a = jnp.where(in_a, base + rank, -1.0)
    pos_b = jnp.where(in_a, -1.0, base + rank - half)

    row = row_ref[...].astype(F32) + 1.0
    high = floor_div(row, 128)
    low = row - high * 128
    where_row = lax.broadcasted_iota(jnp.int32, (128, tokens), 0)
    zeros = jnp.zeros((128 - tail, tokens), BF)
    for ext, first in ((ext_a, 0), (ext_b, 2)):
        ext[:main, :] = grad_ref[:main, :]
        ext[main + 128:, :] = jnp.where(
            where_row == first, high, jnp.where(where_row == first + 1, low, 0.0)).astype(BF)
    ext_a[main:main + tail, :] = grad_ref[main:, :]
    ext_a[main + tail:main + 128, :] = zeros
    ext_b[main:main + 128 - tail, :] = zeros
    ext_b[main + 128 - tail:main + 128, :] = grad_ref[main:, :]

    def place(g):
        line = iota((gs, 1), 0) + (g * gs).astype(F32)
        return onehot(line, pos_a), onehot(line, pos_b)

    def copy_out(step):
        return pltpu.make_async_remote_copy(
            src_ref=send.at[step], dst_ref=recv.at[step], send_sem=send_sem.at[step],
            recv_sem=recv_sem.at[step], device_id=ahead(step), device_id_type=MESH)

    def copy_back(step):
        return pltpu.make_async_remote_copy(
            src_ref=answer.at[step], dst_ref=returned.at[step], send_sem=back_sem.at[step],
            recv_sem=ret_sem.at[step], device_id=behind(step), device_id_type=MESH)

    def stay_out():
        return pltpu.make_async_copy(send.at[step_self], recv.at[step_self], recv_sem.at[step_self])

    def stay_back():
        return pltpu.make_async_copy(
            answer.at[step_self], returned.at[step_self], ret_sem.at[step_self])

    def start_group(g, remote, local):
        def one(i, carry):
            step = g * group + i

            @pl.when(step != step_self)
            def _():
                remote(step).start()

            @pl.when(step == step_self)
            def _():
                local().start()
            return carry
        lax.fori_loop(0, group, one, 0)

    def wait_group(g, remote, local):
        def one(i, carry):
            step = g * group + i

            @pl.when(step != step_self)
            def _():
                remote(step).wait_recv()

            @pl.when(step == step_self)
            def _():
                local().wait()
            return carry
        lax.fori_loop(0, group, one, 0)

    def wait_sent(remote):
        def one(step, carry):
            @pl.when(step != step_self)
            def _():
                remote(step).wait_send()
            return carry
        lax.fori_loop(0, n, one, 0)

    pl.semaphore_wait(barrier, n - 1)

    def pack(buffer, g, part_a, part_b):
        span = pl.ds(g * group, group)
        buffer[span, :, 0:main] = part_a[:, :main].astype(BF).reshape(group, half, main)
        buffer[span, :, main:2 * main] = part_b[:, :main].astype(BF).reshape(group, half, main)
        both = part_a[:, main:] + part_b[:, main:]
        buffer[span, :, 2 * main:] = both.astype(BF).reshape(group, half, both.shape[1])

    def scatter(g, carry):
        place_a, place_b = place(g)
        pack(send, g, nt(place_a, ext_a[...]), nt(place_b, ext_b[...]))
        start_group(g, copy_out, stay_out)
        return carry

    lax.fori_loop(0, groups, scatter, 0)
    total[...] = jnp.zeros_like(total)
    fresh[...] = jnp.zeros_like(fresh)

    def load_lhs(buffer, g):
        block = buffer[pl.ds(g * group, group)]
        block = block.reshape(gs, block.shape[2])
        tails = block[:, 2 * main:2 * main + 128].T
        lhs[:main, :gs] = block[:, :main].T
        lhs[:main, gs:] = block[:, main:2 * main].T
        lhs[main:, :gs] = tails[:tail]
        lhs[main:, gs:] = tails[128 - tail:]

    def row_columns(g):
        block = recv[pl.ds(g * group, group), :, 2 * main + 128:]
        block = block.reshape(gs, 128).astype(F32)
        return (block[:, 0:1] * 128 + block[:, 1:2] - 1.0,
                block[:, 2:3] * 128 + block[:, 3:4] - 1.0)

    tile = 512

    def collect(g, carry):
        wait_group(g, copy_out, stay_out)
        load_lhs(recv, g)
        row_a, row_b = row_columns(g)

        def part(r, inner):
            span = pl.ds(pl.multiple_of(r * tile, tile), tile)
            line = iota((1, tile), 1) + (r * tile).astype(F32)
            hot = jnp.concatenate([onehot(row_a, line), onehot(row_b, line)], axis=0)
            total[:, span] += jnp.dot(lhs[...], hot, preferred_element_type=F32)
            return inner

        lax.fori_loop(0, rows // tile, part, 0)
        return carry

    lax.fori_loop(0, groups, collect, 0)
    load.wait()

    def update(r, carry):
        span = pl.ds(pl.multiple_of(r * tile, tile), tile)
        summed = total[:, span]
        grown = accum_ref[:, span] + jnp.sum(summed * summed, axis=0, keepdims=True) * (1.0 / width)
        new_accum_ref[:, span] = grown
        moved = table[:, span] - summed * (0.5 / (jnp.sqrt(grown) + 1e-08))
        new_table[:, span] = moved
        short = moved.astype(BF)
        zero = jnp.zeros((128 - tail, tile), BF)
        new_a[:main, span] = short[:main]
        new_b[:main, span] = short[:main]
        new_a[main:main + tail, span] = short[main:]
        new_a[main + tail:, span] = zero
        new_b[main:main + 128 - tail, span] = zero
        new_b[main + 128 - tail:, span] = short[main:]
        return carry

    lax.fori_loop(0, rows // tile, update, 0)
    store = pltpu.make_async_copy(new_table, new_table_ref, out_sem)
    store.start()

    def reply(g, carry):
        row_a, row_b = row_columns(g)
        ans_a[...] = jnp.zeros_like(ans_a)
        ans_b[...] = jnp.zeros_like(ans_b)

        def part(r, inner):
            span = pl.ds(pl.multiple_of(r * tile, tile), tile)
            line = iota((1, tile), 1) + (r * tile).astype(F32)
            ans_a[...] += nt(onehot(row_a, line), new_a[:, span])
            ans_b[...] += nt(onehot(row_b, line), new_b[:, span])
            return inner

        lax.fori_loop(0, rows // tile, part, 0)
        pack(answer, g, ans_a[...], ans_b[...])
        start_group(g, copy_back, stay_back)
        return carry

    lax.fori_loop(0, groups, reply, 0)

    def finish(g, carry):
        wait_group(g, copy_back, stay_back)
        load_lhs(returned, g)
        fresh[...] += jnp.dot(
            lhs[...], jnp.concatenate(place(g), axis=0), preferred_element_type=F32)
        return carry

    lax.fori_loop(0, groups, finish, 0)
    fresh_ref[...] = fresh[...].astype(BF)
    wait_sent(copy_out)
    wait_sent(copy_back)
    store.wait()


def body(token_grad, token_owner, token_row, table, accum):
    sizes = tuple(lax.axis_size(axis) for axis in AXES)
    n = sizes[0] * sizes[1] * sizes[2]
    tokens, width = token_grad.shape
    rows = table.shape[0]
    half = max(16, tokens // n)
    group = max(1, 256 // half)
    gs = group * half
    main = width // 128 * 128
    vmem = pl.BlockSpec(memory_space=pltpu.VMEM)
    hbm = pl.BlockSpec(memory_space=pl.ANY)
    dma = pltpu.SemaphoreType.DMA
    new_table, new_accum, fresh = pl.pallas_call(
        functools.partial(kernel, sizes, half),
        out_shape=(
            jax.ShapeDtypeStruct((width, rows), F32),
            jax.ShapeDtypeStruct((1, rows), F32),
            jax.ShapeDtypeStruct((width, tokens), BF),
        ),
        in_specs=[vmem, vmem, vmem, hbm, vmem],
        out_specs=(hbm, vmem, vmem),
        scratch_shapes=[
            pltpu.VMEM((main + 256, tokens), BF),
            pltpu.VMEM((main + 256, tokens), BF),
            pltpu.VMEM((n, half, 2 * main + 256), BF),
            pltpu.VMEM((n, half, 2 * main + 256), BF),
            pltpu.VMEM((width, rows), F32),
            pltpu.VMEM((width, rows), F32),
            pltpu.VMEM((width, rows), F32),
            pltpu.VMEM((main + 128, rows), BF),
            pltpu.VMEM((main + 128, rows), BF),
            pltpu.VMEM((width, 2 * gs), BF),
            pltpu.VMEM((gs, main + 128), F32),
            pltpu.VMEM((gs, main + 128), F32),
            pltpu.VMEM((n, half, 2 * main + 128), BF),
            pltpu.VMEM((n, half, 2 * main + 128), BF),
            pltpu.VMEM((width, tokens), F32),
            dma((n,)), dma((n,)), dma((n,)), dma((n,)), dma, dma,
        ],
        compiler_params=pltpu.CompilerParams(
            collective_id=0, has_side_effects=True, vmem_limit_bytes=63 * 1024 * 1024),
    )(token_grad.T, token_owner.reshape(1, tokens), token_row.reshape(1, tokens), table.T,
      accum.reshape(1, rows))
    return new_table.T, new_accum.reshape(rows), fresh.T


def solution(mesh):
    return jax.shard_map(
        body,
        mesh=mesh,
        in_specs=(P(AXES, None), P(AXES, None), P(AXES), P(AXES, None), P(AXES)),
        out_specs=(P(AXES, None), P(AXES), P(AXES, None)),
        check_vma=False,
    )
```

```python
import functools

import jax
import jax.numpy as jnp
from jax import lax
from jax.experimental import pallas as pl
from jax.experimental.pallas import tpu as pltpu
from jax.sharding import PartitionSpec as P

AXES = ("gx", "gy", "gz")
BF, F32 = jnp.bfloat16, jnp.float32
MESH = pl.DeviceIdType.MESH


def iota(shape, axis):
    return lax.broadcasted_iota(jnp.int32, shape, axis).astype(F32)


def floor_div(value, by):
    return jnp.floor((value + 0.5) * (1.0 / by))


def onehot(column, line):
    return jnp.where(column == line, 1.0, 0.0).astype(BF)


def nt(left, right):
    return lax.dot_general(left, right, (((1,), (1,)), ((), ())), preferred_element_type=F32)


def kernel(sizes, half, grad_ref, owner_ref, row_ref, table_ref, accum_ref,
           new_table_ref, new_accum_ref, fresh_ref,
           ext, send_row, recv_row, send, recv, total, table, new_table, short_table,
           lhs, ans, answer, returned, fresh,
           row_out_sem, row_in_sem, send_sem, recv_sem, back_sem, ret_sem, table_sem, out_sem):
    xs, ys, zs = sizes
    n = xs * ys * zs
    width, tokens = grad_ref.shape
    rows = table.shape[1]
    main = width // 128 * 128
    tail = width - main
    group = max(1, 128 // half)
    groups = n // group
    gs = group * half
    step_self = ys - 1
    me = tuple(lax.axis_index(axis) for axis in AXES)

    def delta(step):
        b = ys - 1 - lax.rem(step, ys)
        return lax.rem(step // (ys * zs), xs), b, lax.rem(step // ys, zs)

    def ahead(step):
        return tuple(lax.rem(m + d, s) for m, d, s in zip(me, delta(step), sizes))

    def behind(step):
        return tuple(lax.rem(m + s - d, s) for m, d, s in zip(me, delta(step), sizes))

    barrier = pltpu.get_barrier_semaphore()

    def greet(step, carry):
        @pl.when(step != step_self)
        def _():
            pl.semaphore_signal(barrier, inc=1, device_id=ahead(step), device_id_type=MESH)
        return carry

    lax.fori_loop(0, n, greet, 0)
    load = pltpu.make_async_copy(table_ref, table, table_sem)
    load.start()

    owner = owner_ref[...].astype(F32)
    step = iota((n, tokens), 0)
    rest = floor_div(step, ys)
    b_part = ys - 1 - (step - rest * ys)
    a_part = floor_div(rest, zs)
    c_part = rest - a_part * zs

    def turn(part, m, size):
        moved = part + m.astype(F32)
        return jnp.where(moved >= size, moved - size, moved)

    named = (turn(a_part, me[0], xs) * ys + turn(b_part, me[1], ys)) * zs + turn(c_part, me[2], zs)
    match = jnp.where(named == owner, 1.0, 0.0)
    earlier = jnp.where(iota((tokens, tokens), 0) < iota((tokens, tokens), 1), 1.0, 0.0).astype(BF)
    before = jnp.dot(match.astype(BF), earlier, preferred_element_type=F32)
    rank = jnp.sum(match * before, axis=0, keepdims=True)
    base = jnp.sum(match * step, axis=0, keepdims=True) * half
    in_a = rank < half
    pos_a = jnp.where(in_a, base + rank, -1.0)
    pos_b = jnp.where(in_a, -1.0, base + rank - half)

    row = row_ref[...].astype(F32) + 1.0
    high = floor_div(row, 128)
    low = row - high * 128
    lane = jnp.where(iota((128, tokens), 0) == rank, 1.0, 0.0).astype(BF)
    rows_out = nt((match * high).astype(BF), lane) * 128.0 + nt((match * low).astype(BF), lane)
    send_row[...] = rows_out.reshape(n, 1, 128)
    zeros = jnp.zeros((128 - tail, tokens), BF)
    ext[:width, :] = grad_ref[...]
    ext[width:, :] = zeros

    def place(g):
        line = iota((gs, 1), 0) + (g * gs).astype(F32)
        return jnp.concatenate([onehot(line, pos_a), onehot(line, pos_b)], axis=0)

    def copy_out(step):
        return pltpu.make_async_remote_copy(
            src_ref=send.at[step], dst_ref=recv.at[step], send_sem=send_sem.at[step],
            recv_sem=recv_sem.at[step], device_id=ahead(step), device_id_type=MESH)

    def copy_row(step):
        return pltpu.make_async_remote_copy(
            src_ref=send_row.at[step], dst_ref=recv_row.at[step], send_sem=row_out_sem.at[step],
            recv_sem=row_in_sem.at[step], device_id=ahead(step), device_id_type=MESH)

    def stay_row():
        return pltpu.make_async_copy(
            send_row.at[step_self], recv_row.at[step_self], row_in_sem.at[step_self])

    def copy_back(step):
        return pltpu.make_async_remote_copy(
            src_ref=answer.at[step], dst_ref=returned.at[step], send_sem=back_sem.at[step],
            recv_sem=ret_sem.at[step], device_id=behind(step), device_id_type=MESH)

    def stay_out():
        return pltpu.make_async_copy(send.at[step_self], recv.at[step_self], recv_sem.at[step_self])

    def stay_back():
        return pltpu.make_async_copy(
            answer.at[step_self], returned.at[step_self], ret_sem.at[step_self])

    def start_range(first, count, remote, local):
        def one(i, carry):
            step = first + i

            @pl.when(step != step_self)
            def _():
                remote(step).start()

            @pl.when(step == step_self)
            def _():
                local().start()
            return carry
        lax.fori_loop(0, count, one, 0)

    def wait_range(first, count, remote, local):
        def one(i, carry):
            step = first + i

            @pl.when(step != step_self)
            def _():
                remote(step).wait_recv()

            @pl.when(step == step_self)
            def _():
                local().wait()
            return carry
        lax.fori_loop(0, count, one, 0)

    def wait_sent(remote):
        def one(step, carry):
            @pl.when(step != step_self)
            def _():
                remote(step).wait_send()
            return carry
        lax.fori_loop(0, n, one, 0)

    pl.semaphore_wait(barrier, n - 1)
    start_range(0, n, copy_row, stay_row)

    def pack(buffer, g, parts):
        part_a, part_b = parts[:gs], parts[gs:]
        span = pl.ds(g * group, group)
        buffer[span, :, 0:main] = part_a[:, :main].astype(BF).reshape(group, half, main)
        buffer[span, :, main:2 * main] = part_b[:, :main].astype(BF).reshape(group, half, main)
        both = part_a[:, main:] + pltpu.roll(part_b[:, main:], 128 - tail, axis=1)
        buffer[span, :, 2 * main:] = both.astype(BF).reshape(group, half, both.shape[1])

    def scatter(g, carry):
        pack(send, g, nt(place(g), ext[...]))
        start_range(g * group, group, copy_out, stay_out)
        return carry

    lax.fori_loop(0, groups, scatter, 0)
    total[...] = jnp.zeros_like(total)
    fresh[...] = jnp.zeros_like(fresh)

    def load_lhs(buffer, g):
        block = buffer[pl.ds(g * group, group)]
        block = block.reshape(gs, block.shape[2])
        tails = block[:, 2 * main:2 * main + 128].T
        lhs[:main, :gs] = block[:, :main].T
        lhs[:main, gs:] = block[:, main:2 * main].T
        lhs[main:, :gs] = tails[:tail]
        lhs[main:, gs:] = tails[128 - tail:]

    def row_columns(g):
        block = recv_row[pl.ds(g * group, group)].reshape(group, 128)
        high = floor_div(block, 128)
        slot = iota((gs, group), 0)
        pick = jnp.where(floor_div(slot, half) == iota((gs, group), 1), 1.0, 0.0).astype(BF)
        spread = (jnp.dot(pick, high.astype(BF), preferred_element_type=F32) * 128.0
                  + jnp.dot(pick, (block - high * 128).astype(BF), preferred_element_type=F32))
        slot = iota((gs, 128), 0)
        slot = slot - floor_div(slot, half) * half
        lanes = iota((gs, 128), 1)
        return tuple(
            jnp.sum(jnp.where(lanes == slot + first, spread, 0.0), axis=1, keepdims=True) - 1.0
            for first in (0, half))

    tile = 2048

    def collect(g, carry):
        wait_range(g * group, group, copy_out, stay_out)
        load_lhs(recv, g)
        row_a, row_b = row_columns(g)

        def part(r, inner):
            span = pl.ds(pl.multiple_of(r * tile, tile), tile)
            line = iota((1, tile), 1) + (r * tile).astype(F32)
            hot = jnp.concatenate([onehot(row_a, line), onehot(row_b, line)], axis=0)
            total[:, span] += jnp.dot(lhs[...], hot, preferred_element_type=F32)
            return inner

        lax.fori_loop(0, rows // tile, part, 0)
        return carry

    wait_range(0, n, copy_row, stay_row)
    lax.fori_loop(0, groups, collect, 0)
    load.wait()

    def update(r, carry):
        span = pl.ds(pl.multiple_of(r * tile, tile), tile)
        summed = total[:, span]
        grown = accum_ref[:, span] + jnp.sum(summed * summed, axis=0, keepdims=True) * (1.0 / width)
        new_accum_ref[:, span] = grown
        moved = table[:, span] - summed * (0.5 / (jnp.sqrt(grown) + 1e-08))
        new_table[:, span] = moved
        short = moved.astype(BF)
        zero = jnp.zeros((128 - tail, tile), BF)
        short_table[:width, span] = short
        short_table[width:, span] = zero
        return carry

    lax.fori_loop(0, rows // tile, update, 0)
    store = pltpu.make_async_copy(new_table, new_table_ref, out_sem)
    store.start()

    def reply(g, carry):
        row_a, row_b = row_columns(g)
        ans[...] = jnp.zeros_like(ans)

        def part(r, inner):
            span = pl.ds(pl.multiple_of(r * tile, tile), tile)
            line = iota((1, tile), 1) + (r * tile).astype(F32)
            hot = jnp.concatenate([onehot(row_a, line), onehot(row_b, line)], axis=0)
            ans[...] += nt(hot, short_table[:, span])
            return inner

        lax.fori_loop(0, rows // tile, part, 0)
        pack(answer, g, ans[...])
        start_range(g * group, group, copy_back, stay_back)
        return carry

    lax.fori_loop(0, groups, reply, 0)

    def finish(g, carry):
        wait_range(g * group, group, copy_back, stay_back)
        load_lhs(returned, g)
        fresh[...] += jnp.dot(
            lhs[...], place(g), preferred_element_type=F32)
        return carry

    lax.fori_loop(0, groups, finish, 0)
    fresh_ref[...] = fresh[...].astype(BF)
    wait_sent(copy_row)
    wait_sent(copy_out)
    wait_sent(copy_back)
    store.wait()


def body(token_grad, token_owner, token_row, table, accum):
    sizes = tuple(lax.axis_size(axis) for axis in AXES)
    n = sizes[0] * sizes[1] * sizes[2]
    tokens, width = token_grad.shape
    rows = table.shape[0]
    half = max(16, tokens // n)
    group = max(1, 128 // half)
    gs = group * half
    main = width // 128 * 128
    vmem = pl.BlockSpec(memory_space=pltpu.VMEM)
    hbm = pl.BlockSpec(memory_space=pl.ANY)
    dma = pltpu.SemaphoreType.DMA
    new_table, new_accum, fresh = pl.pallas_call(
        functools.partial(kernel, sizes, half),
        out_shape=(
            jax.ShapeDtypeStruct((width, rows), F32),
            jax.ShapeDtypeStruct((1, rows), F32),
            jax.ShapeDtypeStruct((width, tokens), BF),
        ),
        in_specs=[vmem, vmem, vmem, hbm, vmem],
        out_specs=(hbm, vmem, vmem),
        scratch_shapes=[
            pltpu.VMEM((main + 128, tokens), BF),
            pltpu.VMEM((n, 1, 128), F32),
            pltpu.VMEM((n, 1, 128), F32),
            pltpu.VMEM((n, half, 2 * main + 128), BF),
            pltpu.VMEM((n, half, 2 * main + 128), BF),
            pltpu.VMEM((width, rows), F32),
            pltpu.VMEM((width, rows), F32),
            pltpu.VMEM((width, rows), F32),
            pltpu.VMEM((main + 128, rows), BF),
            pltpu.VMEM((width, 2 * gs), BF),
            pltpu.VMEM((2 * gs, main + 128), F32),
            pltpu.VMEM((n, half, 2 * main + 128), BF),
            pltpu.VMEM((n, half, 2 * main + 128), BF),
            pltpu.VMEM((width, tokens), F32),
            dma((n,)), dma((n,)), dma((n,)), dma((n,)), dma((n,)), dma((n,)), dma, dma,
        ],
        compiler_params=pltpu.CompilerParams(
            collective_id=0, has_side_effects=True, vmem_limit_bytes=63 * 1024 * 1024),
    )(token_grad.T, token_owner.reshape(1, tokens), token_row.reshape(1, tokens), table.T,
      accum.reshape(1, rows))
    return new_table.T, new_accum.reshape(rows), fresh.T


def solution(mesh):
    return jax.shard_map(
        body,
        mesh=mesh,
        in_specs=(P(AXES, None), P(AXES, None), P(AXES), P(AXES, None), P(AXES)),
        out_specs=(P(AXES, None), P(AXES), P(AXES, None)),
        check_vma=False,
    )
```
